256 devices in a mesh: rad: 64 (over y, z, core), ell: 4 (over x).
Axes of the slice: x: 4, y: 4, z: 8, core: 2. Of those that a mesh axis runs over, the one named last changes fastest.
Arguments:
- field: bfloat16 [512, 128, 512], P('rad', 'ell'), may hold values from -6 to 6
- projection: bfloat16 [512, 128, 256], P('rad', 'ell'), may hold values from -0.75 to 0.75
- ell_ids: int32 [128], P('ell'), may hold values from 0 to 255, as said below
Outputs:
- share: float32 [128, 256], P('ell', 'rad')
- crest: float32 [128, 256], P('ell', 'rad')
The draws below stay inside these ranges and needn't reach their ends.
Inputs may be any that keep to these rules, and one draw needn't show every extreme that they name: `ell_ids`: distinct and ascending.
All inputs are finite; a program needn't handle non-finite values.
Results may differ from the reference program's by a relative error of at most 0.0003.
Values may be sent and summed in bfloat16 or wider, within the bound.
No kernel may reach another device: no remote copies, remote signals or barrier semaphores. Data moves between devices by JAX's collectives and lax.ppermute only.
A program may use at most 64 MiB of HBM per device.

```python
import jax
import jax.numpy as jnp

LMAX = 256
M = 512
R = 512
N = 256
ELLS = 128


def draw_ell_ids(key, part):
    chosen = jax.random.permutation(jax.random.fold_in(key, 11), LMAX)[:ELLS]
    return jnp.sort(chosen).astype(jnp.int32)


def spiked(result, own_key, source, target, shards_of, factor):
    owner, partner = [(jnp.arange(result.shape[dim]) // (result.shape[dim] // shards_of)).reshape([-1 if axis == dim else 1 for axis in range(result.ndim)]) for dim in (source, target)]
    chosen = jax.random.permutation(own_key, shards_of)[partner]
    strong = (owner == chosen) | (owner == (partner + shards_of // 2) % shards_of)
    return jnp.where(strong, factor * result, result)


def level_of(rng, dims, pieces, least, largest):
    factor_of, own = 1.0, jax.random.fold_in(rng, 6)
    for axis_at, shards_of in pieces:
        draws = jnp.exp(jax.random.uniform(jax.random.fold_in(own, axis_at), (shards_of,), jnp.float32, least / len(pieces), largest / len(pieces)))
        factor_of = factor_of * jnp.repeat(draws, dims[axis_at] // shards_of).reshape([-1 if axis == axis_at else 1 for axis in range(len(dims))])
    return factor_of


def gaussian(own_key, shape, spread, reach, shards=(), kind=jnp.bfloat16):
    values = spread * jax.random.normal(own_key, shape, jnp.float32)
    if shards:
        values = values * level_of(own_key, shape, shards, -0.22, 0.18)
    return jnp.clip(values, -reach, reach).astype(kind)


def heavy_noise(own_key, extent, deviation, most, cuts, heavy, kind=jnp.bfloat16):
    result = deviation * jax.random.normal(own_key, extent, jnp.float32)
    if cuts:
        result = result * level_of(own_key, extent, cuts, -0.22, 0.18)
    return jnp.clip(spiked(result, jax.random.fold_in(own_key, 3), *heavy), -most, most).astype(kind)


def setup_inputs(seed: int = 0) -> dict:
    arg_keys = jax.random.split(jax.random.key(seed), 4)
    return {
        "field": gaussian(arg_keys[0], (R, ELLS, M), 1.0, 6.0, ((0, 64), (1, 4))),
        "projection": heavy_noise(arg_keys[1], (R, ELLS, N), R ** -0.5, 0.75, ((0, 64), (1, 4)), (0, 2, 64, 4.0)),
        "ell_ids": draw_ell_ids(jax.random.fold_in(arg_keys[3], 71), 0),
    }


def reference(field, projection, ell_ids):
    coef = jnp.einsum("rem,ren->emn", field.astype(jnp.float32), projection.astype(jnp.float32))
    slots = jnp.arange(M, dtype=jnp.int32)
    valid = (slots[None, :] < (2 * ell_ids[:, None] + 1)).astype(jnp.float32)
    energy = jnp.sum(valid[:, :, None] * coef * coef, axis=1)
    peak = jnp.max(valid[:, :, None] * jnp.abs(coef), axis=1)
    column = jnp.sum(energy, axis=0) + 1e-6
    top = jnp.max(peak, axis=0) + 1e-6
    share = ELLS * energy / column[None, :]
    crest = peak / top[None, :]
    return share, crest
```

```python
import jax
import jax.numpy as jnp
from jax import lax
from jax.sharding import PartitionSpec as P


def per_device(field, projection, ell_ids):
    radii, ells, slots = field.shape
    modes = projection.shape[2]
    owners = lax.axis_size("rad")
    parts = owners // ells
    groups = lax.axis_size("ell")
    width = slots // parts
    me = lax.axis_index("rad")
    turned = field.reshape(radii, ells, parts, width).transpose(1, 2, 0, 3)
    shared = jnp.broadcast_to(
        projection.transpose(1, 0, 2)[:, None], (ells, parts, radii, modes)
    )
    sent = jnp.concatenate([turned, shared], axis=-1).reshape(owners, radii, width + modes)
    got = lax.all_to_all(sent, "rad", 0, 0, tiled=True).reshape(owners * radii, width + modes)
    coef = lax.dot_general(
        got[:, :width],
        got[:, width:],
        (((0,), (0,)), ((), ())),
        preferred_element_type=jnp.float32,
    )
    ell = lax.dynamic_index_in_dim(ell_ids, me // parts, keepdims=False)
    slot = (me % parts) * width + jnp.arange(width, dtype=jnp.int32)
    valid = (slot < 2 * ell + 1).astype(jnp.float32)[:, None]
    energy_part = jnp.sum(valid * coef * coef, axis=0)
    peak_part = jnp.max(valid * jnp.abs(coef), axis=0)
    own = modes // owners
    both = jnp.concatenate(
        [energy_part.reshape(owners, own), peak_part.reshape(owners, own)], axis=-1
    )
    both = jnp.broadcast_to(both[:, None], (owners, groups, 2 * own))
    both = both.reshape(owners * groups, 2 * own)
    spread = lax.all_to_all(both, ("rad", "ell"), 0, 0, tiled=True)
    spread = spread.reshape(ells, parts, groups, 2 * own)
    energy = jnp.sum(spread[..., :own], axis=1)
    peak = jnp.max(spread[..., own:], axis=1)
    column = jnp.sum(energy, axis=(0, 1)) + 1e-06
    top = jnp.max(peak, axis=(0, 1)) + 1e-06
    group = lax.axis_index("ell")
    energy = lax.dynamic_index_in_dim(energy, group, axis=1, keepdims=False)
    peak = lax.dynamic_index_in_dim(peak, group, axis=1, keepdims=False)
    share = ells * groups * energy / column[None, :]
    crest = peak / top[None, :]
    return (share, crest)


def solution(mesh):
    in_specs = (P("rad", "ell", None), P("rad", "ell", None), P("ell"))
    out_specs = (P("ell", "rad"), P("ell", "rad"))
    return jax.shard_map(
        per_device, mesh=mesh, in_specs=in_specs, out_specs=out_specs, check_vma=False
    )
```

```python
import jax
import jax.numpy as jnp
from jax import lax
from jax.sharding import Mesh
from jax.sharding import PartitionSpec as P

CORES = 2
CHIPS_Y = 4
CHIPS = ("y", "z")
WHERE = ("y", "z", "core")


def pick(modes, own, core):
    source = lax.broadcasted_iota(jnp.int32, (modes, modes // CORES), 0)
    target = lax.broadcasted_iota(jnp.int32, (modes, modes // CORES), 1)
    wanted = (target // own) * (own * CORES) + core * own + target % own
    return (source == wanted).astype(jnp.bfloat16)


def per_device(field, projection, ell_ids):
    radii, ells, slots = field.shape
    modes = projection.shape[2]
    groups = lax.axis_size("ell")
    own = modes // (ells * CORES)
    core = lax.axis_index("core")
    chip = lax.axis_index(CHIPS)
    group = lax.axis_index("ell")
    ell = lax.dynamic_index_in_dim(ell_ids, chip, keepdims=False)
    valid = (jnp.arange(slots, dtype=jnp.int32) < 2 * ell + 1).astype(jnp.float32)
    other = pick(modes, own, 1 - core)
    mine = pick(modes, own, core)
    sent = jnp.concatenate([field.transpose(1, 0, 2), projection.transpose(1, 0, 2)], axis=-1)
    sent, valid, other, mine, group = lax.optimization_barrier((sent, valid, other, mine, group))
    got = lax.all_to_all(sent, CHIPS, 0, 0, tiled=True).reshape(ells * radii, slots + modes)
    values, weights = got[:, :slots], got[:, slots:]

    def half(selection):
        chosen = lax.dot(weights, selection, preferred_element_type=jnp.float32)
        return lax.dot_general(
            values,
            chosen.astype(jnp.bfloat16),
            (((0,), (0,)), ((), ())),
            preferred_element_type=jnp.float32,
        )

    away = lax.ppermute(half(other), "core", [(0, 1), (1, 0)])
    coef = half(mine) + away
    energy = jnp.sum(valid[:, None] * coef * coef, axis=0)
    peak = jnp.max(valid[:, None] * jnp.abs(coef), axis=0)
    both = jnp.concatenate([energy.reshape(ells, own), peak.reshape(ells, own)], axis=-1)
    both = jnp.broadcast_to(both[:, None], (ells, groups, 2 * own))
    both = both.reshape(ells * groups, 2 * own)
    both, group = lax.optimization_barrier((both, group))
    spread = lax.all_to_all(both, (*CHIPS, "ell"), 0, 0, tiled=True)
    spread, group = lax.optimization_barrier((spread, group))
    spread = spread.reshape(ells, groups, 2 * own)
    column = jnp.sum(spread[..., :own], axis=(0, 1)) + 1e-06
    top = jnp.max(spread[..., own:], axis=(0, 1)) + 1e-06
    held = lax.dynamic_index_in_dim(spread, group, axis=1, keepdims=False)
    share = ells * groups * held[:, :own] / column[None, :]
    crest = held[:, own:] / top[None, :]
    return (share, crest)


def solution(mesh):
    devices = mesh.devices.reshape(CHIPS_Y, -1, CORES, mesh.shape["ell"])
    fine = Mesh(devices, ("y", "z", "core", "ell"))
    in_specs = (P(WHERE, "ell", None), P(WHERE, "ell", None), P("ell"))
    out_specs = (P("ell", WHERE), P("ell", WHERE))
    return jax.shard_map(
        per_device, mesh=fine, in_specs=in_specs, out_specs=out_specs, check_vma=False
    )
```

```python
import jax
import jax.numpy as jnp
from jax import lax
from jax.sharding import Mesh
from jax.sharding import PartitionSpec as P

CORES = 2
CHIPS_Y = 4
CHIPS = ("y", "z")
WHERE = ("y", "z", "core")


def pick(modes, own, core):
    source = lax.broadcasted_iota(jnp.int32, (modes, modes // CORES), 0)
    target = lax.broadcasted_iota(jnp.int32, (modes, modes // CORES), 1)
    wanted = (target // own) * (own * CORES) + core * own + target % own
    return (source == wanted).astype(jnp.bfloat16)


def per_device(field, projection, ell_ids):
    radii, ells, slots = field.shape
    modes = projection.shape[2]
    groups = lax.axis_size("ell")
    own = modes // (ells * CORES)
    core = lax.axis_index("core")
    chip = lax.axis_index(CHIPS)
    group = lax.axis_index("ell")
    other = pick(modes, own, 1 - core)
    mine = pick(modes, own, core)
    sent = jnp.concatenate([field.transpose(1, 0, 2), projection.transpose(1, 0, 2)], axis=-1)
    sent, other, mine, group, chip = lax.optimization_barrier((sent, other, mine, group, chip))
    got = lax.all_to_all(sent, CHIPS, 0, 0, tiled=True)
    got, chip = lax.optimization_barrier((got, chip))
    got = got.reshape(ells * radii, slots + modes)
    values, weights = got[:, :slots], got[:, slots:]

    def half(selection):
        chosen = lax.dot(weights, selection, preferred_element_type=jnp.float32)
        return lax.dot_general(
            values,
            chosen.astype(jnp.bfloat16),
            (((0,), (0,)), ((), ())),
            preferred_element_type=jnp.float32,
        )

    leaving, ell_ids, chip = lax.optimization_barrier((half(other), ell_ids, chip))
    away = lax.ppermute(leaving, "core", [(0, 1), (1, 0)])
    kept = lax.optimization_barrier(half(mine))
    ell = lax.dynamic_index_in_dim(ell_ids, chip, keepdims=False)
    valid = (jnp.arange(slots, dtype=jnp.int32) < 2 * ell + 1).astype(jnp.float32)
    coef = kept + away
    energy = jnp.sum(valid[:, None] * coef * coef, axis=0)
    peak = jnp.max(valid[:, None] * jnp.abs(coef), axis=0)
    both = jnp.concatenate([energy.reshape(ells, own), peak.reshape(ells, own)], axis=-1)
    both = jnp.broadcast_to(both[:, None], (ells, groups, 2 * own))
    both = both.reshape(ells * groups, 2 * own)
    both, group = lax.optimization_barrier((both, group))
    spread = lax.all_to_all(both, (*CHIPS, "ell"), 0, 0, tiled=True)
    spread, group = lax.optimization_barrier((spread, group))
    spread = spread.reshape(ells, groups, 2 * own)
    column = jnp.sum(spread[..., :own], axis=(0, 1)) + 1e-06
    top = jnp.max(spread[..., own:], axis=(0, 1)) + 1e-06
    held = lax.dynamic_index_in_dim(spread, group, axis=1, keepdims=False)
    share = ells * groups * held[:, :own] / column[None, :]
    crest = held[:, own:] / top[None, :]
    return (share, crest)


def solution(mesh):
    devices = mesh.devices.reshape(CHIPS_Y, -1, CORES, mesh.shape["ell"])
    fine = Mesh(devices, ("y", "z", "core", "ell"))
    in_specs = (P(WHERE, "ell", None), P(WHERE, "ell", None), P("ell"))
    out_specs = (P("ell", WHERE), P("ell", WHERE))
    return jax.shard_map(
        per_device, mesh=fine, in_specs=in_specs, out_specs=out_specs, check_vma=False
    )
```

```python
import jax
import jax.numpy as jnp
from jax import lax
from jax.sharding import Mesh
from jax.sharding import PartitionSpec as P

CORES = 2
CHIPS_Y = 4
CHIPS = ("y", "z")
WHERE = ("y", "z", "core")


def pick(modes, own, core):
    source = lax.broadcasted_iota(jnp.int32, (modes, modes // CORES), 0)
    target = lax.broadcasted_iota(jnp.int32, (modes, modes // CORES), 1)
    wanted = (target // own) * (own * CORES) + core * own + target % own
    return (source == wanted).astype(jnp.bfloat16)


def per_device(field, projection, ell_ids):
    radii, ells, slots = field.shape
    modes = projection.shape[2]
    groups = lax.axis_size("ell")
    own = modes // (ells * CORES)
    core = lax.axis_index("core")
    chip = lax.axis_index(CHIPS)
    group = lax.axis_index("ell")
    other = pick(modes, own, 1 - core)
    mine = pick(modes, own, core)
    sent = jnp.concatenate([field.transpose(1, 0, 2), projection.transpose(1, 0, 2)], axis=-1)
    needed = (jnp.arange(slots, dtype=jnp.int32) + 1) // 2
    sent, other, mine, needed, group, chip = lax.optimization_barrier(
        (sent, other, mine, needed, group, chip)
    )
    got = lax.all_to_all(sent, CHIPS, 0, 0, tiled=True)
    got, chip = lax.optimization_barrier((got, chip))
    got = got.reshape(ells * radii, slots + modes)
    values, weights = got[:, :slots], got[:, slots:]

    def half(selection):
        chosen = lax.dot(weights, selection, preferred_element_type=jnp.float32)
        return lax.dot_general(
            values,
            chosen.astype(jnp.bfloat16),
            (((0,), (0,)), ((), ())),
            preferred_element_type=jnp.float32,
        )

    leaving, chip = lax.optimization_barrier((half(other), chip))
    away = lax.ppermute(leaving, "core", [(0, 1), (1, 0)])
    kept = lax.optimization_barrier(half(mine))
    here = jnp.arange(ells, dtype=jnp.int32)[None, :] == chip
    inside = needed[:, None] <= ell_ids[None, :]
    valid = jnp.sum((here & inside).astype(jnp.float32), axis=1)
    coef = kept + away
    energy = jnp.sum(valid[:, None] * coef * coef, axis=0)
    peak = jnp.max(valid[:, None] * jnp.abs(coef), axis=0)
    both = jnp.concatenate([energy.reshape(ells, own), peak.reshape(ells, own)], axis=-1)
    both = jnp.broadcast_to(both[:, None], (ells, groups, 2 * own))
    both = both.reshape(ells * groups, 2 * own)
    both, group = lax.optimization_barrier((both, group))
    spread = lax.all_to_all(both, (*CHIPS, "ell"), 0, 0, tiled=True)
    spread, group = lax.optimization_barrier((spread, group))
    spread = spread.reshape(ells, groups, 2 * own)
    column = jnp.sum(spread[..., :own], axis=(0, 1)) + 1e-06
    top = jnp.max(spread[..., own:], axis=(0, 1)) + 1e-06
    held = lax.dynamic_index_in_dim(spread, group, axis=1, keepdims=False)
    share = ells * groups * held[:, :own] / column[None, :]
    crest = held[:, own:] / top[None, :]
    return (share, crest)


def solution(mesh):
    devices = mesh.devices.reshape(CHIPS_Y, -1, CORES, mesh.shape["ell"])
    fine = Mesh(devices, ("y", "z", "core", "ell"))
    in_specs = (P(WHERE, "ell", None), P(WHERE, "ell", None), P("ell"))
    out_specs = (P("ell", WHERE), P("ell", WHERE))
    return jax.shard_map(
        per_device, mesh=fine, in_specs=in_specs, out_specs=out_specs, check_vma=False
    )
```

```python
import functools

import jax
import jax.numpy as jnp
from jax import lax
from jax.experimental import pallas as pl
from jax.experimental.pallas import tpu as pltpu
from jax.sharding import Mesh
from jax.sharding import PartitionSpec as P

CORES = 2
CHIPS_Y = 4
SCOPED = 4 * 2**20
CHIPS = ("y", "z")
WHERE = ("y", "z", "core")


def pick(modes, own, core):
    source = lax.broadcasted_iota(jnp.int32, (modes, modes // CORES), 0)
    target = lax.broadcasted_iota(jnp.int32, (modes, modes // CORES), 1)
    wanted = (target // own) * (own * CORES) + core * own + target % own
    return (source == wanted).astype(jnp.bfloat16)


def spread_kernel(own, groups, kept, away, ids, out):
    coef = kept[...] + away[...]
    here = lax.broadcasted_iota(jnp.int32, ids.shape, 1) == lax.axis_index(CHIPS)
    ell = jnp.sum(jnp.where(here, ids[...], 0), axis=1, keepdims=True)
    slot = lax.broadcasted_iota(jnp.int32, coef.shape, 0)
    chosen = jnp.where(slot < 2 * ell + 1, coef, 0.0)
    energy = jnp.sum(chosen * coef, axis=0, keepdims=True)
    peak = jnp.max(jnp.abs(chosen), axis=0, keepdims=True)
    count = out.shape[0] // groups
    width = energy.shape[1]
    lane = lax.broadcasted_iota(jnp.int32, (count, width), 1)
    mine = lane // own == lax.broadcasted_iota(jnp.int32, (count, width), 0)
    energies = jnp.where(mine, energy, 0.0)
    peaks = jnp.where(mine, peak, 0.0)
    shift = own
    while shift < width:
        energies = energies + pltpu.roll(energies, shift, 1)
        peaks = peaks + pltpu.roll(peaks, shift, 1)
        shift *= 2
    rows = jnp.where(lane < own, energies, peaks)
    for group in range(groups):
        out[pl.ds(group * count, count)] = rows


def scale_kernel(own, ells, groups, spread, share, crest):
    values = spread[...]
    column = jnp.sum(values, axis=0, keepdims=True) + 1e-06
    top = jnp.max(values, axis=0, keepdims=True) + 1e-06
    first = pl.multiple_of(lax.axis_index("ell") * ells, ells)
    held = spread[pl.ds(first, ells)]
    lane = lax.broadcasted_iota(jnp.int32, held.shape, 1)
    scaled = jnp.where(lane < own, ells * groups * held / column, held / top)
    turned = scaled.T
    share[...] = turned[:own]
    crest[...] = turned[own : 2 * own]


def per_device(field, projection, ell_ids):
    radii, ells, slots = field.shape
    modes = projection.shape[2]
    groups = lax.axis_size("ell")
    own = modes // (ells * CORES)
    core = lax.axis_index("core")
    other = pick(modes, own, 1 - core)
    mine = pick(modes, own, core)
    sent = jnp.concatenate([field.transpose(1, 0, 2), projection.transpose(1, 0, 2)], axis=-1)
    sent, other, mine = lax.optimization_barrier((sent, other, mine))
    got = lax.all_to_all(sent, CHIPS, 0, 0, tiled=True)
    got, ell_ids = lax.optimization_barrier((got, ell_ids))
    got = got.reshape(ells * radii, slots + modes)
    values, weights = got[:, :slots], got[:, slots:]

    def half(selection):
        chosen = lax.dot(weights, selection, preferred_element_type=jnp.float32)
        return lax.dot_general(
            values,
            chosen.astype(jnp.bfloat16),
            (((0,), (0,)), ((), ())),
            preferred_element_type=jnp.float32,
        )

    away = lax.ppermute(half(other), "core", [(0, 1), (1, 0)])
    kept = lax.optimization_barrier(half(mine))
    both = pl.pallas_call(
        functools.partial(spread_kernel, own, groups),
        out_shape=jax.ShapeDtypeStruct((ells * groups, modes // CORES), jnp.float32),
        in_specs=[pl.BlockSpec(memory_space=pltpu.VMEM)] * 3,
        out_specs=pl.BlockSpec(memory_space=pltpu.VMEM),
        compiler_params=pltpu.CompilerParams(vmem_limit_bytes=SCOPED),
    )(kept, away, ell_ids[None])
    spread = lax.all_to_all(both, ("ell", *CHIPS), 0, 0, tiled=True)
    shape = jax.ShapeDtypeStruct((own, ells), jnp.float32)
    share, crest = pl.pallas_call(
        functools.partial(scale_kernel, own, ells, groups),
        out_shape=(shape, shape),
        in_specs=[pl.BlockSpec(memory_space=pltpu.VMEM)],
        out_specs=(pl.BlockSpec(memory_space=pltpu.VMEM),) * 2,
        compiler_params=pltpu.CompilerParams(vmem_limit_bytes=SCOPED),
    )(spread)
    return (share.T, crest.T)


def solution(mesh):
    devices = mesh.devices.reshape(CHIPS_Y, -1, CORES, mesh.shape["ell"])
    fine = Mesh(devices, ("y", "z", "core", "ell"))
    in_specs = (P(WHERE, "ell", None), P(WHERE, "ell", None), P("ell"))
    out_specs = (P("ell", WHERE), P("ell", WHERE))
    return jax.shard_map(
        per_device, mesh=fine, in_specs=in_specs, out_specs=out_specs, check_vma=False
    )
```

```python
import functools

import jax
import jax.numpy as jnp
from jax import lax
from jax.experimental import pallas as pl
from jax.experimental.pallas import tpu as pltpu
from jax.sharding import Mesh
from jax.sharding import PartitionSpec as P

CORES = 2
CHIPS_Y = 4
SCOPED = 4 * 2**20
CHIPS = ("y", "z")
WHERE = ("y", "z", "core")


def pick(modes, own, core):
    source = lax.broadcasted_iota(jnp.int32, (modes, modes // CORES), 0)
    target = lax.broadcasted_iota(jnp.int32, (modes, modes // CORES), 1)
    wanted = (target // own) * (own * CORES) + core * own + target % own
    return (source == wanted).astype(jnp.bfloat16)


def spread_kernel(groups, kept, away, ids, out):
    coef = kept[...] + away[...]
    here = lax.broadcasted_iota(jnp.int32, ids.shape, 1) == lax.axis_index(CHIPS)
    ell = jnp.sum(jnp.where(here, ids[...], 0), axis=1, keepdims=True)
    slot = lax.broadcasted_iota(jnp.int32, coef.shape, 0)
    chosen = jnp.where(slot < 2 * ell + 1, coef, 0.0)
    energy = jnp.sum(chosen * coef, axis=0, keepdims=True)
    peak = jnp.max(jnp.abs(chosen), axis=0, keepdims=True)
    width = energy.shape[1]
    fold = width // 2
    lane = lax.broadcasted_iota(jnp.int32, energy.shape, 1)
    low = jnp.where(lane < fold, energy, pltpu.roll(peak, fold, 1))
    high = jnp.where(lane < fold, pltpu.roll(energy, fold, 1), peak)
    count = out.shape[0] // groups // 2
    for group in range(groups):
        out[pl.ds(2 * group * count, count)] = jnp.broadcast_to(low, (count, width))
        out[pl.ds((2 * group + 1) * count, count)] = jnp.broadcast_to(high, (count, width))


def scale_kernel(own, ells, groups, spread, share, crest, turned):
    column = jnp.sum(spread[...], axis=0, keepdims=True) + 1e-06
    top = jnp.max(spread[...], axis=0, keepdims=True) + 1e-06
    first = pl.multiple_of(lax.axis_index("ell") * ells, ells)
    held = spread[pl.ds(first, ells)]
    fold = held.shape[1] // 2
    lane = lax.broadcasted_iota(jnp.int32, held.shape, 1)
    turned[...] = jnp.where(lane < fold, ells * groups * held / column, held / top).T
    place = lax.rem(lax.axis_index(CHIPS) * own, fold)
    share[...] = turned[pl.ds(place, own)]
    crest[...] = turned[pl.ds(place + fold, own)]


def per_device(field, projection, ell_ids):
    radii, ells, slots = field.shape
    modes = projection.shape[2]
    groups = lax.axis_size("ell")
    own = modes // (ells * CORES)
    core = lax.axis_index("core")
    other = pick(modes, own, 1 - core)
    mine = pick(modes, own, core)
    sent = jnp.concatenate([field.transpose(1, 0, 2), projection.transpose(1, 0, 2)], axis=-1)
    sent, other, mine = lax.optimization_barrier((sent, other, mine))
    got = lax.all_to_all(sent, CHIPS, 0, 0, tiled=True)
    got, ell_ids = lax.optimization_barrier((got, ell_ids))
    got = got.reshape(ells * radii, slots + modes)
    values, weights = got[:, :slots], got[:, slots:]

    def half(selection):
        chosen = lax.dot(weights, selection, preferred_element_type=jnp.float32)
        return lax.dot_general(
            values,
            chosen.astype(jnp.bfloat16),
            (((0,), (0,)), ((), ())),
            preferred_element_type=jnp.float32,
        )

    away = lax.ppermute(half(other), "core", [(0, 1), (1, 0)])
    kept = lax.optimization_barrier(half(mine))
    both = pl.pallas_call(
        functools.partial(spread_kernel, groups),
        out_shape=jax.ShapeDtypeStruct((ells * groups, modes // CORES), jnp.float32),
        in_specs=[pl.BlockSpec(memory_space=pltpu.VMEM)] * 3,
        out_specs=pl.BlockSpec(memory_space=pltpu.VMEM),
        compiler_params=pltpu.CompilerParams(vmem_limit_bytes=SCOPED),
    )(kept, away, ell_ids[None])
    spread = lax.all_to_all(both, ("ell", *CHIPS), 0, 0, tiled=True)
    shape = jax.ShapeDtypeStruct((own, ells), jnp.float32)
    share, crest = pl.pallas_call(
        functools.partial(scale_kernel, own, ells, groups),
        out_shape=(shape, shape),
        in_specs=[pl.BlockSpec(memory_space=pltpu.VMEM)],
        out_specs=(pl.BlockSpec(memory_space=pltpu.VMEM),) * 2,
        scratch_shapes=[pltpu.VMEM((modes // CORES, ells), jnp.float32)],
        compiler_params=pltpu.CompilerParams(vmem_limit_bytes=SCOPED),
    )(spread)
    return (share.T, crest.T)


def solution(mesh):
    devices = mesh.devices.reshape(CHIPS_Y, -1, CORES, mesh.shape["ell"])
    fine = Mesh(devices, ("y", "z", "core", "ell"))
    in_specs = (P(WHERE, "ell", None), P(WHERE, "ell", None), P("ell"))
    out_specs = (P("ell", WHERE), P("ell", WHERE))
    return jax.shard_map(
        per_device, mesh=fine, in_specs=in_specs, out_specs=out_specs, check_vma=False
    )
```

```python
import functools
import itertools

import jax
import jax.numpy as jnp
from jax import lax
from jax.experimental import pallas as pl
from jax.experimental.pallas import tpu as pltpu
from jax.sharding import Mesh
from jax.sharding import PartitionSpec as P

CORES = 2
CHIPS_Y = 4
SCOPED = 4 * 2**20
CHIPS = ("y", "z")
WHERE = ("y", "z", "core")


def farthest_first(*sizes):
    def hops(place):
        return sum(min(at, size - at) for at, size in zip(place, sizes))

    return sorted(itertools.product(*map(range, sizes)), key=hops)[::-1]


def turn_of(order, index):
    turn = jnp.int32(0)
    for k, member in enumerate(order):
        turn = jnp.where(index == member, k, turn)
    return turn


def pick(modes, own, core):
    source = lax.broadcasted_iota(jnp.int32, (modes, modes // CORES), 0)
    target = lax.broadcasted_iota(jnp.int32, (modes, modes // CORES), 1)
    wanted = (target // own) * (own * CORES) + core * own + target % own
    return (source == wanted).astype(jnp.bfloat16)


def spread_kernel(groups, order, kept, away, ids, out):
    coef = kept[...] + away[...]
    turn = turn_of(order, lax.axis_index(CHIPS))
    here = lax.broadcasted_iota(jnp.int32, ids.shape, 1) == turn
    ell = jnp.sum(jnp.where(here, ids[...], 0), axis=1, keepdims=True)
    slot = lax.broadcasted_iota(jnp.int32, coef.shape, 0)
    chosen = jnp.where(slot < 2 * ell + 1, coef, 0.0)
    energy = jnp.sum(chosen * coef, axis=0, keepdims=True)
    peak = jnp.max(jnp.abs(chosen), axis=0, keepdims=True)
    width = energy.shape[1]
    fold = width // 2
    lane = lax.broadcasted_iota(jnp.int32, energy.shape, 1)
    halves = (
        jnp.where(lane < fold, energy, pltpu.roll(peak, fold, 1)),
        jnp.where(lane < fold, pltpu.roll(energy, fold, 1), peak),
    )
    uppers = [2 * chip // len(order) for chip in order]
    for group in range(groups):
        at = group * len(order)
        for upper, run in itertools.groupby(uppers):
            count = len(list(run))
            out[pl.ds(at, count)] = jnp.broadcast_to(halves[upper], (count, width))
            at += count


def scale_kernel(own, order, spread, share, crest, turned):
    groups = len(order)
    ells = spread.shape[0] // groups
    column = jnp.sum(spread[...], axis=0, keepdims=True) + 1e-06
    top = jnp.max(spread[...], axis=0, keepdims=True) + 1e-06
    first = pl.multiple_of(turn_of(order, lax.axis_index("ell")) * ells, ells)
    held = spread[pl.ds(first, ells)]
    fold = held.shape[1] // 2
    lane = lax.broadcasted_iota(jnp.int32, held.shape, 1)
    turned[...] = jnp.where(lane < fold, ells * groups * held / column, held / top).T
    place = lax.rem(lax.axis_index(CHIPS) * own, fold)
    share[...] = turned[pl.ds(place, own)]
    crest[...] = turned[pl.ds(place + fold, own)]


def per_device(field, projection, ell_ids):
    radii, ells, slots = field.shape
    modes = projection.shape[2]
    groups = lax.axis_size("ell")
    chips = [y * lax.axis_size("z") + z for y, z in farthest_first(*map(lax.axis_size, CHIPS))]
    planes = [x for (x,) in farthest_first(groups)]
    near = [[chip * CORES + c for chip in chips] for c in range(CORES)]
    wide = [
        [(chip * CORES + c) * groups + plane for plane in planes for chip in chips]
        for c in range(CORES)
    ]
    own = modes // (ells * CORES)
    core = lax.axis_index("core")
    other = pick(modes, own, 1 - core)
    mine = pick(modes, own, core)
    sent = jnp.concatenate([field.transpose(1, 0, 2), projection.transpose(1, 0, 2)], axis=-1)
    sent, other, mine = lax.optimization_barrier((sent, other, mine))
    got = lax.all_to_all(sent, WHERE, 0, 0, tiled=True, axis_index_groups=near)
    got, ell_ids = lax.optimization_barrier((got, ell_ids))
    got = got.reshape(ells * radii, slots + modes)
    values, weights = got[:, :slots], got[:, slots:]

    def half(selection):
        chosen = lax.dot(weights, selection, preferred_element_type=jnp.float32)
        return lax.dot_general(
            values,
            chosen.astype(jnp.bfloat16),
            (((0,), (0,)), ((), ())),
            preferred_element_type=jnp.float32,
        )

    away = lax.ppermute(half(other), "core", [(0, 1), (1, 0)])
    kept = lax.optimization_barrier(half(mine))
    both = pl.pallas_call(
        functools.partial(spread_kernel, groups, chips),
        out_shape=jax.ShapeDtypeStruct((ells * groups, modes // CORES), jnp.float32),
        in_specs=[pl.BlockSpec(memory_space=pltpu.VMEM)] * 3,
        out_specs=pl.BlockSpec(memory_space=pltpu.VMEM),
        compiler_params=pltpu.CompilerParams(vmem_limit_bytes=SCOPED),
    )(kept, away, ell_ids[None])
    spread = lax.all_to_all(
        both, (*WHERE, "ell"), 0, 0, tiled=True, axis_index_groups=wide
    )
    shape = jax.ShapeDtypeStruct((own, ells), jnp.float32)
    share, crest = pl.pallas_call(
        functools.partial(scale_kernel, own, planes),
        out_shape=(shape, shape),
        in_specs=[pl.BlockSpec(memory_space=pltpu.VMEM)],
        out_specs=(pl.BlockSpec(memory_space=pltpu.VMEM),) * 2,
        scratch_shapes=[pltpu.VMEM((modes // CORES, ells), jnp.float32)],
        compiler_params=pltpu.CompilerParams(vmem_limit_bytes=SCOPED),
    )(spread)
    return (share.T, crest.T)


def solution(mesh):
    devices = mesh.devices.reshape(CHIPS_Y, -1, CORES, mesh.shape["ell"])
    fine = Mesh(devices, ("y", "z", "core", "ell"))
    in_specs = (P(WHERE, "ell", None), P(WHERE, "ell", None), P("ell"))
    out_specs = (P("ell", WHERE), P("ell", WHERE))
    return jax.shard_map(
        per_device, mesh=fine, in_specs=in_specs, out_specs=out_specs, check_vma=False
    )
```

```python
import functools
import itertools

import jax
import jax.numpy as jnp
from jax import lax
from jax.experimental import pallas as pl
from jax.experimental.pallas import tpu as pltpu
from jax.sharding import Mesh
from jax.sharding import PartitionSpec as P

CORES = 2
CHIPS_Y = 4
SCOPED = 4 * 2**20
SUBLANES = 8
CHIPS = ("y", "z")
WHERE = ("y", "z", "core")


def farthest_first(*sizes):
    def hops(place):
        return sum(min(at, size - at) for at, size in zip(place, sizes))

    return sorted(itertools.product(*map(range, sizes)), key=hops)[::-1]


def turn_of(order, index):
    turn = jnp.int32(0)
    for k, member in enumerate(order):
        turn = jnp.where(index == member, k, turn)
    return turn


def pick(modes, own, core):
    source = lax.broadcasted_iota(jnp.int32, (modes, modes // CORES), 0)
    target = lax.broadcasted_iota(jnp.int32, (modes, modes // CORES), 1)
    wanted = (target // own) * (own * CORES) + core * own + target % own
    return (source == wanted).astype(jnp.bfloat16)


def spread_kernel(groups, order, kept, away, ids, out):
    coef = kept[...] + away[...]
    turn = turn_of(order, lax.axis_index(CHIPS))
    here = lax.broadcasted_iota(jnp.int32, ids.shape, 1) == turn
    ell = jnp.sum(jnp.where(here, ids[...], 0), axis=1, keepdims=True)
    slot = lax.broadcasted_iota(jnp.int32, coef.shape, 0)
    chosen = jnp.where(slot < 2 * ell + 1, coef, 0.0)
    energy = jnp.sum(chosen * coef, axis=0, keepdims=True)
    peak = jnp.max(jnp.abs(chosen), axis=0, keepdims=True)
    width = energy.shape[1]
    fold = width // 2
    lane = lax.broadcasted_iota(jnp.int32, energy.shape, 1)
    halves = (
        jnp.where(lane < fold, energy, pltpu.roll(peak, fold, 1)),
        jnp.where(lane < fold, pltpu.roll(energy, fold, 1), peak),
    )
    uppers = [2 * chip // len(order) for chip in order]
    for group in range(groups):
        at = group * len(order)
        for upper, run in itertools.groupby(uppers):
            count = len(list(run))
            out[pl.ds(at, count)] = jnp.broadcast_to(halves[upper], (count, width))
            at += count


def scale_kernel(own, order, spread, share, crest, turned):
    groups = len(order)
    ells = spread.shape[0] // groups
    column = jnp.sum(spread[...], axis=0, keepdims=True) + 1e-06
    top = jnp.max(spread[...], axis=0, keepdims=True) + 1e-06
    first = pl.multiple_of(turn_of(order, lax.axis_index("ell")) * ells, ells)
    held = spread[pl.ds(first, ells)]
    fold = held.shape[1] // 2
    lane = lax.broadcasted_iota(jnp.int32, held.shape, 1)
    scaled = jnp.where(lane < fold, ells * groups * held / column, held / top)
    turned[pl.ds(0, 2 * fold)] = scaled.T
    place = lax.rem(lax.axis_index(CHIPS) * own, fold)
    share[...] = turned[pl.ds(place, own)]
    crest[...] = turned[pl.ds(place + fold, own)]


def per_device(field, projection, ell_ids):
    radii, ells, slots = field.shape
    modes = projection.shape[2]
    groups = lax.axis_size("ell")
    chips = [y * lax.axis_size("z") + z for y, z in farthest_first(*map(lax.axis_size, CHIPS))]
    planes = [x for (x,) in farthest_first(groups)]
    near = [[chip * CORES + c for chip in chips] for c in range(CORES)]
    wide = [
        [(chip * CORES + c) * groups + plane for plane in planes for chip in chips]
        for c in range(CORES)
    ]
    own = modes // (ells * CORES)
    core = lax.axis_index("core")
    other = pick(modes, own, 1 - core)
    mine = pick(modes, own, core)
    sent = jnp.concatenate([field.transpose(1, 0, 2), projection.transpose(1, 0, 2)], axis=-1)
    sent, other, mine = lax.optimization_barrier((sent, other, mine))
    got = lax.all_to_all(sent, WHERE, 0, 0, tiled=True, axis_index_groups=near)
    got, ell_ids = lax.optimization_barrier((got, ell_ids))
    got = got.reshape(ells * radii, slots + modes)
    values, weights = got[:, :slots], got[:, slots:]

    def half(selection):
        chosen = lax.dot(weights, selection, preferred_element_type=jnp.float32)
        return lax.dot_general(
            values,
            chosen.astype(jnp.bfloat16),
            (((0,), (0,)), ((), ())),
            preferred_element_type=jnp.float32,
        )

    away = lax.ppermute(half(other), "core", [(0, 1), (1, 0)])
    kept = lax.optimization_barrier(half(mine))
    both = pl.pallas_call(
        functools.partial(spread_kernel, groups, chips),
        out_shape=jax.ShapeDtypeStruct((ells * groups, modes // CORES), jnp.float32),
        in_specs=[pl.BlockSpec(memory_space=pltpu.VMEM)] * 3,
        out_specs=pl.BlockSpec(memory_space=pltpu.VMEM),
        compiler_params=pltpu.CompilerParams(vmem_limit_bytes=SCOPED),
    )(kept, away, ell_ids[None])
    spread = lax.all_to_all(
        both, (*WHERE, "ell"), 0, 0, tiled=True, axis_index_groups=wide
    )
    shape = jax.ShapeDtypeStruct((own, ells), jnp.float32)
    share, crest = pl.pallas_call(
        functools.partial(scale_kernel, own, planes),
        out_shape=(shape, shape),
        in_specs=[pl.BlockSpec(memory_space=pltpu.VMEM)],
        out_specs=(pl.BlockSpec(memory_space=pltpu.VMEM),) * 2,
        scratch_shapes=[pltpu.VMEM((modes // CORES + SUBLANES, ells), jnp.float32)],
        compiler_params=pltpu.CompilerParams(vmem_limit_bytes=SCOPED),
    )(spread)
    return (share.T, crest.T)


def solution(mesh):
    devices = mesh.devices.reshape(CHIPS_Y, -1, CORES, mesh.shape["ell"])
    fine = Mesh(devices, ("y", "z", "core", "ell"))
    in_specs = (P(WHERE, "ell", None), P(WHERE, "ell", None), P("ell"))
    out_specs = (P("ell", WHERE), P("ell", WHERE))
    return jax.shard_map(
        per_device, mesh=fine, in_specs=in_specs, out_specs=out_specs, check_vma=False
    )
```

```python
import functools
import itertools

import jax
import jax.numpy as jnp
from jax import lax
from jax.experimental import pallas as pl
from jax.experimental.pallas import tpu as pltpu
from jax.sharding import Mesh
from jax.sharding import PartitionSpec as P

CORES = 2
CHIPS_Y = 4
SCOPED = 4 * 2**20
SUBLANES = 8
CHIPS = ("y", "z")
WHERE = ("y", "z", "core")


def farthest_first(*sizes):
    def hops(place):
        return sum(min(at, size - at) for at, size in zip(place, sizes))

    return sorted(itertools.product(*map(range, sizes)), key=hops)[::-1]


def turn_of(order, index):
    turn = jnp.int32(0)
    for k, member in enumerate(order):
        turn = jnp.where(index == member, k, turn)
    return turn


def pick(modes, own, core):
    source = lax.broadcasted_iota(jnp.int32, (modes, modes // CORES), 0)
    target = lax.broadcasted_iota(jnp.int32, (modes, modes // CORES), 1)
    wanted = (target // own) * (own * CORES) + core * own + target % own
    return (source == wanted).astype(jnp.bfloat16)


def spread_kernel(groups, order, kept, away, ids, out):
    coef = kept[...] + away[...]
    turn = turn_of(order, lax.axis_index(CHIPS))
    here = lax.broadcasted_iota(jnp.int32, ids.shape, 1) == turn
    ell = jnp.sum(jnp.where(here, ids[...], 0), axis=1, keepdims=True)
    slot = lax.broadcasted_iota(jnp.int32, coef.shape, 0)
    chosen = jnp.where(slot < 2 * ell + 1, coef, 0.0)
    energy = jnp.sum(chosen * coef, axis=0, keepdims=True)
    peak = jnp.max(jnp.abs(chosen), axis=0, keepdims=True)
    width = energy.shape[1]
    fold = width // 2
    lane = lax.broadcasted_iota(jnp.int32, energy.shape, 1)
    halves = (
        jnp.where(lane < fold, energy, pltpu.roll(peak, fold, 1)),
        jnp.where(lane < fold, pltpu.roll(energy, fold, 1), peak),
    )
    uppers = [2 * chip // len(order) for chip in order]
    for group in range(groups):
        at = group * len(order)
        for upper, run in itertools.groupby(uppers):
            count = len(list(run))
            out[pl.ds(at, count)] = jnp.broadcast_to(halves[upper], (count, width))
            at += count


def scale_kernel(own, order, spread, share, crest, turned):
    groups = len(order)
    ells = spread.shape[0] // groups
    values = spread[...]
    fold = values.shape[1] // 2
    lane = lax.broadcasted_iota(jnp.int32, (1, 2 * fold), 1)
    column = jnp.sum(values, axis=0, keepdims=True)
    top = jnp.max(values, axis=0, keepdims=True)
    below = jnp.where(lane < fold, column, top) + 1e-06
    above = jnp.where(lane < fold, float(ells * groups), 1.0)
    first = pl.multiple_of(turn_of(order, lax.axis_index("ell")) * ells, ells)
    scaled = above * spread[pl.ds(first, ells)] / below
    turned[pl.ds(0, 2 * fold)] = scaled.T
    place = lax.rem(lax.axis_index(CHIPS) * own, fold)
    share[...] = turned[pl.ds(place, own)]
    crest[...] = turned[pl.ds(place + fold, own)]


def per_device(field, projection, ell_ids):
    radii, ells, slots = field.shape
    modes = projection.shape[2]
    groups = lax.axis_size("ell")
    chips = [y * lax.axis_size("z") + z for y, z in farthest_first(*map(lax.axis_size, CHIPS))]
    planes = [x for (x,) in farthest_first(groups)]
    near = [[chip * CORES + c for chip in chips] for c in range(CORES)]
    wide = [
        [(chip * CORES + c) * groups + plane for plane in planes for chip in chips]
        for c in range(CORES)
    ]
    own = modes // (ells * CORES)
    core = lax.axis_index("core")
    other = pick(modes, own, 1 - core)
    mine = pick(modes, own, core)
    sent = jnp.concatenate([field.transpose(1, 0, 2), projection.transpose(1, 0, 2)], axis=-1)
    sent, other, mine = lax.optimization_barrier((sent, other, mine))
    got = lax.all_to_all(sent, WHERE, 0, 0, tiled=True, axis_index_groups=near)
    got, ell_ids = lax.optimization_barrier((got, ell_ids))
    got = got.reshape(ells * radii, slots + modes)
    values, weights = got[:, :slots], got[:, slots:]

    def half(selection):
        chosen = lax.dot(weights, selection, preferred_element_type=jnp.float32)
        return lax.dot_general(
            values,
            chosen.astype(jnp.bfloat16),
            (((0,), (0,)), ((), ())),
            preferred_element_type=jnp.float32,
        )

    away = lax.ppermute(half(other), "core", [(0, 1), (1, 0)])
    kept = lax.optimization_barrier(half(mine))
    both = pl.pallas_call(
        functools.partial(spread_kernel, groups, chips),
        out_shape=jax.ShapeDtypeStruct((ells * groups, modes // CORES), jnp.float32),
        in_specs=[pl.BlockSpec(memory_space=pltpu.VMEM)] * 3,
        out_specs=pl.BlockSpec(memory_space=pltpu.VMEM),
        compiler_params=pltpu.CompilerParams(vmem_limit_bytes=SCOPED),
    )(kept, away, ell_ids[None])
    spread = lax.all_to_all(
        both, (*WHERE, "ell"), 0, 0, tiled=True, axis_index_groups=wide
    )
    shape = jax.ShapeDtypeStruct((own, ells), jnp.float32)
    share, crest = pl.pallas_call(
        functools.partial(scale_kernel, own, planes),
        out_shape=(shape, shape),
        in_specs=[pl.BlockSpec(memory_space=pltpu.VMEM)],
        out_specs=(pl.BlockSpec(memory_space=pltpu.VMEM),) * 2,
        scratch_shapes=[pltpu.VMEM((modes // CORES + SUBLANES, ells), jnp.float32)],
        compiler_params=pltpu.CompilerParams(vmem_limit_bytes=SCOPED),
    )(spread)
    return (share.T, crest.T)


def solution(mesh):
    devices = mesh.devices.reshape(CHIPS_Y, -1, CORES, mesh.shape["ell"])
    fine = Mesh(devices, ("y", "z", "core", "ell"))
    in_specs = (P(WHERE, "ell", None), P(WHERE, "ell", None), P("ell"))
    out_specs = (P("ell", WHERE), P("ell", WHERE))
    return jax.shard_map(
        per_device, mesh=fine, in_specs=in_specs, out_specs=out_specs, check_vma=False
    )
```

```python
import functools
import itertools

import jax
import jax.numpy as jnp
from jax import lax
from jax.experimental import pallas as pl
from jax.experimental.pallas import tpu as pltpu
from jax.sharding import Mesh
from jax.sharding import PartitionSpec as P

CORES = 2
CHIPS_Y = 4
SCOPED = 4 * 2**20
SUBLANES = 8
LEADER = 2
CHIPS = ("y", "z")
WHERE = ("y", "z", "core")


def farthest_first(*sizes):
    def hops(place):
        return sum(min(at, size - at) for at, size in zip(place, sizes))

    return sorted(itertools.product(*map(range, sizes)), key=hops)[::-1]


def turn_of(order, index):
    turn = jnp.int32(0)
    for k, member in enumerate(order):
        turn = jnp.where(index == member, k, turn)
    return turn


def pick(modes, own, core):
    source = lax.broadcasted_iota(jnp.int32, (modes, modes // CORES), 0)
    target = lax.broadcasted_iota(jnp.int32, (modes, modes // CORES), 1)
    wanted = (target // own) * (own * CORES) + core * own + target % own
    return (source == wanted).astype(jnp.bfloat16)


def spread_kernel(groups, order, kept, away, ids, out):
    coef = kept[...] + away[...]
    turn = turn_of(order, lax.axis_index(CHIPS))
    here = lax.broadcasted_iota(jnp.int32, ids.shape, 1) == turn
    ell = jnp.sum(jnp.where(here, ids[...], 0), axis=1, keepdims=True)
    slot = lax.broadcasted_iota(jnp.int32, coef.shape, 0)
    chosen = jnp.where(slot < 2 * ell + 1, coef, 0.0)
    energy = jnp.sum(chosen * coef, axis=0, keepdims=True)
    peak = jnp.max(jnp.abs(chosen), axis=0, keepdims=True)
    width = energy.shape[1]
    fold = width // 2
    lane = lax.broadcasted_iota(jnp.int32, energy.shape, 1)
    halves = (
        jnp.where(lane < fold, energy, pltpu.roll(peak, fold, 1)),
        jnp.where(lane < fold, pltpu.roll(energy, fold, 1), peak),
    )
    uppers = [2 * chip // len(order) for chip in order]
    for group in range(groups):
        at = group * len(order)
        for upper, run in itertools.groupby(uppers):
            count = len(list(run))
            out[pl.ds(at, count)] = jnp.broadcast_to(halves[upper], (count, width))
            at += count


def scale_kernel(own, order, spread, share, crest, turned):
    groups = len(order)
    ells = spread.shape[0] // groups
    column = jnp.sum(spread[...], axis=0, keepdims=True) + 1e-06
    top = jnp.max(spread[...], axis=0, keepdims=True) + 1e-06
    first = pl.multiple_of(turn_of(order, lax.axis_index("ell")) * ells, ells)
    held = spread[pl.ds(first, ells)]
    fold = held.shape[1] // 2
    lane = lax.broadcasted_iota(jnp.int32, held.shape, 1)
    scaled = jnp.where(lane < fold, ells * groups * held / column, held / top)
    turned[pl.ds(0, 2 * fold)] = scaled.T
    place = lax.rem(lax.axis_index(CHIPS) * own, fold)
    share[...] = turned[pl.ds(place, own)]
    crest[...] = turned[pl.ds(place + fold, own)]


def per_device(field, projection, ell_ids):
    radii, ells, slots = field.shape
    modes = projection.shape[2]
    groups = lax.axis_size("ell")
    chips = [y * lax.axis_size("z") + z for y, z in farthest_first(*map(lax.axis_size, CHIPS))]
    chips.insert(0, chips.pop(LEADER))
    planes = [x for (x,) in farthest_first(groups)]
    near = [[chip * CORES + c for chip in chips] for c in range(CORES)]
    wide = [
        [(chip * CORES + c) * groups + plane for plane in planes for chip in chips]
        for c in range(CORES)
    ]
    own = modes // (ells * CORES)
    core = lax.axis_index("core")
    other = pick(modes, own, 1 - core)
    mine = pick(modes, own, core)
    sent = jnp.concatenate([field.transpose(1, 0, 2), projection.transpose(1, 0, 2)], axis=-1)
    sent, other, mine = lax.optimization_barrier((sent, other, mine))
    got = lax.all_to_all(sent, WHERE, 0, 0, tiled=True, axis_index_groups=near)
    got, ell_ids = lax.optimization_barrier((got, ell_ids))
    got = got.reshape(ells * radii, slots + modes)
    values, weights = got[:, :slots], got[:, slots:]

    def half(selection):
        chosen = lax.dot(weights, selection, preferred_element_type=jnp.float32)
        return lax.dot_general(
            values,
            chosen.astype(jnp.bfloat16),
            (((0,), (0,)), ((), ())),
            preferred_element_type=jnp.float32,
        )

    away = lax.ppermute(half(other), "core", [(0, 1), (1, 0)])
    kept = lax.optimization_barrier(half(mine))
    both = pl.pallas_call(
        functools.partial(spread_kernel, groups, chips),
        out_shape=jax.ShapeDtypeStruct((ells * groups, modes // CORES), jnp.float32),
        in_specs=[pl.BlockSpec(memory_space=pltpu.VMEM)] * 3,
        out_specs=pl.BlockSpec(memory_space=pltpu.VMEM),
        compiler_params=pltpu.CompilerParams(vmem_limit_bytes=SCOPED),
    )(kept, away, ell_ids[None])
    spread = lax.all_to_all(
        both, (*WHERE, "ell"), 0, 0, tiled=True, axis_index_groups=wide
    )
    shape = jax.ShapeDtypeStruct((own, ells), jnp.float32)
    share, crest = pl.pallas_call(
        functools.partial(scale_kernel, own, planes),
        out_shape=(shape, shape),
        in_specs=[pl.BlockSpec(memory_space=pltpu.VMEM)],
        out_specs=(pl.BlockSpec(memory_space=pltpu.VMEM),) * 2,
        scratch_shapes=[pltpu.VMEM((modes // CORES + SUBLANES, ells), jnp.float32)],
        compiler_params=pltpu.CompilerParams(vmem_limit_bytes=SCOPED),
    )(spread)
    return (share.T, crest.T)


def solution(mesh):
    devices = mesh.devices.reshape(CHIPS_Y, -1, CORES, mesh.shape["ell"])
    fine = Mesh(devices, ("y", "z", "core", "ell"))
    in_specs = (P(WHERE, "ell", None), P(WHERE, "ell", None), P("ell"))
    out_specs = (P("ell", WHERE), P("ell", WHERE))
    return jax.shard_map(
        per_device, mesh=fine, in_specs=in_specs, out_specs=out_specs, check_vma=False
    )
```

```python
import functools
import itertools

import jax
import jax.numpy as jnp
from jax import lax
from jax.experimental import pallas as pl
from jax.experimental.pallas import tpu as pltpu
from jax.sharding import Mesh
from jax.sharding import PartitionSpec as P

CORES = 2
CHIPS_Y = 4
SCOPED = 4 * 2**20
SUBLANES = 8
LEADER = 2
CHIPS = ("y", "z")
WHERE = ("y", "z", "core")


def farthest_first(*sizes):
    def hops(place):
        return sum(min(at, size - at) for at, size in zip(place, sizes))

    return sorted(itertools.product(*map(range, sizes)), key=hops)[::-1]


def turn_of(order, index):
    turn = jnp.int32(0)
    for k, member in enumerate(order):
        turn = jnp.where(index == member, k, turn)
    return turn


def pick(modes, own, core):
    source = lax.broadcasted_iota(jnp.int32, (modes, modes // CORES), 0)
    target = lax.broadcasted_iota(jnp.int32, (modes, modes // CORES), 1)
    wanted = (target // own) * (own * CORES) + core * own + target % own
    return (source == wanted).astype(jnp.bfloat16)


def spread_kernel(groups, order, kept, away, ids, out):
    coef = kept[...] + away[...]
    turn = turn_of(order, lax.axis_index(CHIPS))
    here = lax.broadcasted_iota(jnp.int32, ids.shape, 1) == turn
    ell = jnp.sum(jnp.where(here, ids[...], 0), axis=1, keepdims=True)
    slot = lax.broadcasted_iota(jnp.int32, coef.shape, 0)
    chosen = jnp.where(slot < 2 * ell + 1, coef, 0.0)
    energy = jnp.sum(chosen * coef, axis=0, keepdims=True)
    peak = jnp.max(jnp.abs(chosen), axis=0, keepdims=True)
    width = energy.shape[1]
    fold = width // 2
    lane = lax.broadcasted_iota(jnp.int32, energy.shape, 1)
    halves = (
        jnp.where(lane < fold, energy, pltpu.roll(peak, fold, 1)),
        jnp.where(lane < fold, pltpu.roll(energy, fold, 1), peak),
    )
    uppers = [2 * chip // len(order) for chip in order]
    for group in range(groups):
        at = group * len(order)
        for upper, run in itertools.groupby(uppers):
            count = len(list(run))
            out[pl.ds(at, count)] = jnp.broadcast_to(halves[upper], (count, width))
            at += count


def scale_kernel(own, order, spread, share, crest, turned):
    groups = len(order)
    ells = spread.shape[0] // groups
    values = spread[...]
    fold = values.shape[1] // 2
    lane = lax.broadcasted_iota(jnp.int32, (1, 2 * fold), 1)
    column = jnp.sum(values, axis=0, keepdims=True)
    top = jnp.max(values, axis=0, keepdims=True)
    below = jnp.where(lane < fold, column, top) + 1e-06
    above = jnp.where(lane < fold, float(ells * groups), 1.0)
    first = pl.multiple_of(turn_of(order, lax.axis_index("ell")) * ells, ells)
    scaled = above * spread[pl.ds(first, ells)] / below
    turned[pl.ds(0, 2 * fold)] = scaled.T
    place = lax.rem(lax.axis_index(CHIPS) * own, fold)
    share[...] = turned[pl.ds(place, own)]
    crest[...] = turned[pl.ds(place + fold, own)]


def per_device(field, projection, ell_ids):
    radii, ells, slots = field.shape
    modes = projection.shape[2]
    groups = lax.axis_size("ell")
    chips = [y * lax.axis_size("z") + z for y, z in farthest_first(*map(lax.axis_size, CHIPS))]
    chips.insert(0, chips.pop(LEADER))
    planes = [x for (x,) in farthest_first(groups)]
    near = [[chip * CORES + c for chip in chips] for c in range(CORES)]
    wide = [
        [(chip * CORES + c) * groups + plane for plane in planes for chip in chips]
        for c in range(CORES)
    ]
    own = modes // (ells * CORES)
    core = lax.axis_index("core")
    other = pick(modes, own, 1 - core)
    mine = pick(modes, own, core)
    sent = jnp.concatenate([field.transpose(1, 0, 2), projection.transpose(1, 0, 2)], axis=-1)
    sent, other, mine = lax.optimization_barrier((sent, other, mine))
    got = lax.all_to_all(sent, WHERE, 0, 0, tiled=True, axis_index_groups=near)
    got, ell_ids = lax.optimization_barrier((got, ell_ids))
    got = got.reshape(ells * radii, slots + modes)
    values, weights = got[:, :slots], got[:, slots:]

    def half(selection):
        chosen = lax.dot(weights, selection, preferred_element_type=jnp.float32)
        return lax.dot_general(
            values,
            chosen.astype(jnp.bfloat16),
            (((0,), (0,)), ((), ())),
            preferred_element_type=jnp.float32,
        )

    away = lax.ppermute(half(other), "core", [(0, 1), (1, 0)])
    kept = lax.optimization_barrier(half(mine))
    both = pl.pallas_call(
        functools.partial(spread_kernel, groups, chips),
        out_shape=jax.ShapeDtypeStruct((ells * groups, modes // CORES), jnp.float32),
        in_specs=[pl.BlockSpec(memory_space=pltpu.VMEM)] * 3,
        out_specs=pl.BlockSpec(memory_space=pltpu.VMEM),
        compiler_params=pltpu.CompilerParams(vmem_limit_bytes=SCOPED),
    )(kept, away, ell_ids[None])
    spread = lax.all_to_all(
        both, (*WHERE, "ell"), 0, 0, tiled=True, axis_index_groups=wide
    )
    shape = jax.ShapeDtypeStruct((own, ells), jnp.float32)
    share, crest = pl.pallas_call(
        functools.partial(scale_kernel, own, planes),
        out_shape=(shape, shape),
        in_specs=[pl.BlockSpec(memory_space=pltpu.VMEM)],
        out_specs=(pl.BlockSpec(memory_space=pltpu.VMEM),) * 2,
        scratch_shapes=[pltpu.VMEM((modes // CORES + SUBLANES, ells), jnp.float32)],
        compiler_params=pltpu.CompilerParams(vmem_limit_bytes=SCOPED),
    )(spread)
    return (share.T, crest.T)


def solution(mesh):
    devices = mesh.devices.reshape(CHIPS_Y, -1, CORES, mesh.shape["ell"])
    fine = Mesh(devices, ("y", "z", "core", "ell"))
    in_specs = (P(WHERE, "ell", None), P(WHERE, "ell", None), P("ell"))
    out_specs = (P("ell", WHERE), P("ell", WHERE))
    return jax.shard_map(
        per_device, mesh=fine, in_specs=in_specs, out_specs=out_specs, check_vma=False
    )
```
